32 devices in a mesh: groups: 2 (over x), seq: 16 (over z, y, core).
Axes of the slice: x: 2, y: 2, z: 4, core: 2. Of those that a mesh axis runs over, the one named last changes fastest.
Arguments:
- queries: bfloat16 [32, 8192], P(('groups', 'seq')), parts along dimension 0, may hold values from -320 to 320, as said below
- span_keys: bfloat16 [32, 1024], P(('groups', 'seq')), parts along dimension 0, may hold values from -6 to 6
- span_values: bfloat16 [32, 1024], P(('groups', 'seq')), parts along dimension 0, may hold values from -6 to 6
- cache_keys: bfloat16 [8192, 1024], P(('groups', 'seq')), parts along dimension 0, may hold values from -6 to 6
- cache_values: bfloat16 [8192, 1024], P(('groups', 'seq')), parts along dimension 0, may hold values from -6 to 6
- page_table: int32 [512], P(('groups', 'seq')), parts along dimension 0, may hold values from 0 to 255, each once
- page_counts: int32 [32], P(('groups', 'seq')), parts along dimension 0, may hold values from 1 to 16, 128 in all
- span_start: int32 [2], P('groups'), parts along dimension 0, may hold values from 2048 to 4095
Outputs:
- attended: bfloat16 [32, 8192], P(('groups', 'seq')), parts along dimension 0
The draws below stay inside these ranges and needn't reach their ends.
There are 2 independent parts, one for each index of `groups`. The reference program is written for one: setup_inputs(seed, part) draws one part's arguments, and reference() takes and returns one part's arrays. A program takes and returns all parts, laid end to end along the dimension named above; each array names one. Nothing has to cross between parts.
Inputs may be any that keep to these rules, and one draw needn't show every extreme that they name: `queries`: queries of every row; in some draws rows differ in scale by a large factor. `page_table`: A permutation of the 256 logical pages. `page_counts`: counts of the shards sum to 128; slots at or beyond a shard's count hold no page; some shard holds 16.
All inputs are finite; a program needn't handle non-finite values.
Results may differ from the reference program's by a relative error of at most 0.02.
The reference program's roundings to bfloat16 on the way count: a program that leaves them out, or rounds other values in their place, can miss the bound.
Values may be sent and summed in bfloat16 or wider, within the bound.
A program may use at most 64 MiB of HBM per device.

```python
import math
import jax
import jax.numpy as jnp
import numpy as np
from jax import lax

H = 64
KVH = 8
HD = 128
PAGE = 16
PAGES_DEV = 16
Q_TOK = 16
N_PAGES = 256
LIVE_PAGES = 128
N_SEQ = 16


def draw_queries(key, part):
    first_key = jax.random.fold_in(jax.random.fold_in(key, 11), 0)
    values = jnp.clip(jax.random.normal(first_key, (Q_TOK, H * HD), jnp.float32), -6.0, 6.0)
    return values.astype(jnp.bfloat16)


def shard_levels(rng, dims, shards, least, high):
    loudness = 1.0
    for dim, blocks in shards:
        draws = jax.random.uniform(jax.random.fold_in(jax.random.fold_in(rng, 6), dim), (blocks,), jnp.float32, least / len(shards), high / len(shards))
        loudness = loudness * jnp.repeat(jnp.exp(draws), dims[dim] // blocks).reshape((-1,) + (1,) * (len(dims) - 1 - dim))
    return loudness


def profile(count, total, reach, lean):
    portions = [(1 << 20) // math.isqrt(standing ** lean) + 1 for standing in range(2, count + 1)]
    rest, counts = total - reach - (count - 1), [1] * (count - 1)
    while rest > 0:
        candidates = [i for i in range(count - 1) if counts[i] < reach]
        whole, budget = sum([portions[i] for i in candidates]), rest
        for i in candidates:
            more = min(reach - counts[i], max(1, budget * portions[i] // whole), rest)
            counts[i] = counts[i] + more
            rest = rest - more
    return np.array([reach] + counts)


def uneven(stream_key, amount, total, bound, lean):
    if amount == 2:
        one = jax.random.randint(stream_key, (), max(1, total - bound), min(bound, total - 1) + 1)
        return jnp.stack([one, total - one])
    sizes = jnp.asarray(profile(amount, total, bound, lean), jnp.int32)
    couples = (amount - 1) // 2
    source_of, receiver = sizes[1:1 + 2 * couples:2], sizes[2:2 + 2 * couples:2]
    slack = jnp.minimum(source_of - 1, bound - receiver)
    moved = jax.random.randint(jax.random.fold_in(stream_key, 1), (couples,), 0, 1 << 20) % (slack + 1)
    sizes = sizes.at[1:1 + 2 * couples:2].set(source_of - moved).at[2:2 + 2 * couples:2].set(receiver + moved)
    return sizes[jax.random.permutation(jax.random.fold_in(stream_key, 2), amount)]


def gaussian(rng, dims, deviation, most, pieces=(), kind=jnp.bfloat16):
    values = deviation * jax.random.normal(rng, dims, jnp.float32)
    if pieces:
        values = values * shard_levels(rng, dims, pieces, -0.22, 0.18)
    return jnp.clip(values, -most, most).astype(kind)


def setup_inputs(seed: int = 0, part: int = 0) -> dict:
    splits = jax.random.split(jax.random.key(seed), 9)
    part_splits = jax.random.split(jax.random.fold_in(splits[8], part), 9)
    queries = draw_queries(jax.random.fold_in(jax.random.fold_in(splits[8], part), 71), part)
    span_keys = gaussian(part_splits[1], (Q_TOK, KVH * HD), 1.0, 6.0, ((0, 16),))
    span_values = gaussian(part_splits[2], (Q_TOK, KVH * HD), 1.0, 6.0, ((0, 16),))
    cache_keys = gaussian(part_splits[3], (N_PAGES * PAGE, KVH * HD), 1.0, 6.0, ((0, 16),))
    cache_values = gaussian(part_splits[4], (N_PAGES * PAGE, KVH * HD), 1.0, 6.0, ((0, 16),))
    page_table = jax.random.permutation(part_splits[5], N_PAGES).astype(jnp.int32)
    page_counts = uneven(part_splits[6], N_SEQ, LIVE_PAGES, PAGES_DEV, 2).astype(jnp.int32)
    span_start = jax.random.randint(part_splits[7], (1,), N_PAGES * PAGE // 2, N_PAGES * PAGE).astype(jnp.int32)
    return dict(queries=queries, span_keys=span_keys, span_values=span_values, cache_keys=cache_keys, cache_values=cache_values, page_table=page_table, page_counts=page_counts, span_start=span_start)


rope_base = 1000000.0
masked_low = -1e30


def rotate(values, positions, heads):
    count_rows = values.shape[0]
    width = values.shape[1] // heads
    half_width = width // 2
    frequency = rope_base ** (-(jnp.arange(half_width, dtype=jnp.float32) * 2.0 / width))
    angles = positions.astype(jnp.float32)[:, None] * frequency[None, :]
    cosine = jnp.cos(angles)[:, None, :]
    sine_part = jnp.sin(angles)[:, None, :]
    headed = values.astype(jnp.float32).reshape(count_rows, heads, width)
    first_half = headed[..., :half_width]
    second_half = headed[..., half_width:]
    turned = jnp.concatenate([first_half * cosine - second_half * sine_part, second_half * cosine + first_half * sine_part], axis=-1)
    return turned.reshape(count_rows, heads * width)


def rounded(values):
    return lax.optimization_barrier(values.astype(jnp.bfloat16)).astype(jnp.float32)


def reference(queries, span_keys, span_values, cache_keys, cache_values, page_table, page_counts, span_start):
    start = span_start[0]
    group = H // KVH
    factor = HD ** -0.5
    key_rows = PAGES_DEV * PAGE
    query_positions = start + jnp.arange(Q_TOK, dtype=jnp.int32)
    query_heads = rounded(rotate(queries, query_positions, H)).reshape(Q_TOK, KVH, group, HD)
    span_heads = rounded(rotate(span_keys, query_positions, KVH)).reshape(Q_TOK, KVH, HD)
    span_vals = span_values.astype(jnp.float32).reshape(Q_TOK, KVH, HD)

    def one_shard(carry, shard_id):
        run_max, run_num, run_den = carry
        keys = lax.dynamic_slice_in_dim(cache_keys, (shard_id * key_rows).astype(jnp.int32), key_rows, 0)
        vals = lax.dynamic_slice_in_dim(cache_values, (shard_id * key_rows).astype(jnp.int32), key_rows, 0)
        table = lax.dynamic_slice_in_dim(page_table, (shard_id * PAGES_DEV).astype(jnp.int32), PAGES_DEV, 0)
        row_ids = jnp.arange(key_rows, dtype=jnp.int32)
        slot_ids = row_ids // PAGE
        positions = jnp.repeat(table, PAGE) * PAGE + row_ids % PAGE
        usable = (slot_ids < page_counts[shard_id]) & (positions < start)
        key_heads = rounded(rotate(keys, positions, KVH)).reshape(key_rows, KVH, HD)
        scores = jnp.einsum('tkgd,skd->ktgs', query_heads, key_heads) * factor
        live = usable[None, None, None, :]
        best = jnp.max(jnp.where(live, scores, masked_low), axis=-1)
        weights = jnp.where(live, jnp.exp(scores - best[..., None]), 0.0)
        denom = jnp.sum(weights, axis=-1)
        numer = jnp.einsum('ktgs,skd->ktgd', rounded(weights), vals.astype(jnp.float32).reshape(key_rows, KVH, HD))
        newest = jnp.maximum(run_max, best)
        old_part = jnp.exp(run_max - newest)
        new_part = jnp.exp(best - newest)
        run_num = run_num * old_part[..., None] + numer * new_part[..., None]
        run_den = run_den * old_part + denom * new_part
        return (newest, run_num, run_den), None

    start_max = jnp.full((KVH, Q_TOK, group), masked_low, jnp.float32)
    start_num = jnp.zeros((KVH, Q_TOK, group, HD), jnp.float32)
    start_den = jnp.zeros((KVH, Q_TOK, group), jnp.float32)
    (pre_max, pre_num, pre_den), unused = lax.scan(one_shard, (start_max, start_num, start_den), jnp.arange(N_SEQ, dtype=jnp.int32))

    self_scores = jnp.einsum('tkgd,skd->ktgs', query_heads, span_heads) * factor
    causal = (jnp.arange(Q_TOK, dtype=jnp.int32)[None, :] <= jnp.arange(Q_TOK, dtype=jnp.int32)[:, None])[None, :, None, :]
    self_max = jnp.max(jnp.where(causal, self_scores, masked_low), axis=-1)
    self_weights = jnp.where(causal, jnp.exp(self_scores - self_max[..., None]), 0.0)
    self_den = jnp.sum(self_weights, axis=-1)
    self_num = jnp.einsum('ktgs,skd->ktgd', rounded(self_weights), span_vals)

    both = jnp.maximum(pre_max, self_max)
    first_weight = jnp.exp(pre_max - both)
    second_weight = jnp.exp(self_max - both)
    total_num = pre_num * first_weight[..., None] + self_num * second_weight[..., None]
    total_den = pre_den * first_weight + self_den * second_weight
    result = total_num / total_den[..., None]
    return result.transpose(1, 0, 2, 3).reshape(Q_TOK, H * HD).astype(jnp.bfloat16)
```

```python
import functools
import math

import jax
import jax.numpy as jnp
import numpy as np
from jax import lax
from jax.experimental import pallas as pl
from jax.experimental.pallas import tpu as pltpu
from jax.sharding import PartitionSpec as P

H = 64
KVH = 8
PAGE = 16
GROUP = H // KVH
HALF_KV = KVH // 2
HALF_H = H // 2
SPAN_PAD = 16

rope_base = 1000000.0
masked_low = -1e30
no_page = float(1 << 20)
MESH = pl.DeviceIdType.MESH


def angle_table(width):
    half = width // 2
    turns = rope_base ** (-(np.arange(half) * 2.0 / width)) / (2.0 * math.pi)
    mant, expo = np.frexp(turns)
    high = np.ldexp(np.floor(mant * 4096.0) / 4096.0, expo)
    rows = np.zeros((8, width), np.float32)
    rows[0] = np.tile(high, 2)
    rows[1] = np.tile(turns - high, 2)
    rows[2] = np.tile(turns, 2)
    rows[3, :half] = 0.25
    return rows


def cos_sin(high_pos, low_pos, tab):
    x = high_pos * tab[0:1]
    x = x - jnp.floor(x + 0.5)
    x = x + (high_pos * tab[1:2] + (low_pos * tab[2:3] + tab[3:4]))
    x = x - jnp.floor(x + 0.5)
    y = jnp.where(x > 0.25, 0.5 - x, jnp.where(x < -0.25, -0.5 - x, x))
    z = y * (2.0 * math.pi)
    z2 = z * z
    acc = jnp.full_like(z2, 1.0 / math.factorial(13))
    for order, sign in ((11, -1.0), (9, 1.0), (7, -1.0), (5, 1.0), (3, -1.0), (1, 1.0)):
        acc = acc * z2 + sign / math.factorial(order)
    both = acc * z
    half = both.shape[-1] // 2
    turned = pltpu.roll(both, half, both.ndim - 1)
    low = lax.broadcasted_iota(jnp.int32, both.shape, both.ndim - 1) < half
    return jnp.where(low, both, turned), jnp.where(low, -turned, both)


def rotate(x, cosine, sine):
    return x * cosine + pltpu.roll(x, x.shape[-1] // 2, x.ndim - 1) * sine


def kernel(
    n, factor,
    table_hbm, counts_hbm, start_hbm,
    q_hbm, sk_hbm, sv_hbm, tab_hbm, keys_hbm, vals_hbm,
    out_ref,
    table_ref, counts_ref, start_ref,
    q_in, sk_in, sv_in, tab_in, keys_raw, vals, keys_rot,
    q_own, q_all, page_own, page_peer, span_own, span_peer,
    num_send, stat_send, num_recv, stat_recv,
    in_sem, peer_send, peer_recv, q_send, q_recv, num_ss, num_rs, stat_ss, stat_rs,
):
    me = lax.axis_index("seq")
    core = lax.rem(me, 2)
    partner = me + 1 - 2 * core
    rows = keys_hbm.shape[0]
    width = tab_hbm.shape[1]
    slots = rows // PAGE
    cols = HALF_KV * width
    chips = n // 2
    unroll = n <= 16 and n & (n - 1) == 0

    def flipped(i):
        peer, bit = me, 1
        while bit < n:
            if i & bit:
                peer = peer + bit * (1 - 2 * lax.rem(me // bit, 2))
            bit *= 2
        return peer

    def forward(i):
        return flipped(i) if unroll else lax.rem(me + i, n)

    def backward(i):
        return flipped(i) if unroll else lax.rem(me + n - i, n)

    def steps(low, high, step):
        if unroll:
            for i in reversed(range(low, high)):
                step(i)
        else:
            def one(i, carry):
                step(i)
                return carry
            lax.fori_loop(low, high, one, 0)

    barrier = pltpu.get_barrier_semaphore()

    def greet(i):
        pl.semaphore_signal(
            barrier, inc=1, device_id={"seq": forward(i)}, device_id_type=MESH
        )

    steps(1, n, greet)

    small = [
        pltpu.make_async_copy(src, dst, in_sem.at[i])
        for i, (src, dst) in enumerate(
            (
                (start_hbm, start_ref), (q_hbm, q_in), (tab_hbm, tab_in), (sk_hbm, sk_in),
                (sv_hbm, sv_in), (table_hbm, table_ref), (counts_hbm, counts_ref),
            )
        )
    ]
    for copy in small:
        copy.start()
    mine = pl.ds(pl.multiple_of(core * cols, cols), cols)
    theirs = pl.ds(pl.multiple_of((1 - core) * cols, cols), cols)
    own_keys = pltpu.make_async_copy(
        keys_hbm.at[:, mine], keys_raw.at[pl.ds(0, rows), :], in_sem.at[7]
    )
    own_vals = pltpu.make_async_copy(
        vals_hbm.at[:, mine], vals.at[pl.ds(0, rows), :], in_sem.at[8]
    )
    own_keys.start()
    own_vals.start()

    def by_head(ref, heads):
        row = ref[...].astype(jnp.float32)
        return jnp.concatenate(
            [row[:, h * width : (h + 1) * width] for h in range(heads)], axis=0
        )

    for copy in small:
        copy.wait()
    start = start_ref[0]
    tab = tab_in[...]
    here = start + me
    high = (here // PAGE) * PAGE
    cosine, sine = cos_sin(
        jnp.full((8, width), high.astype(jnp.float32)),
        jnp.full((8, width), (here - high).astype(jnp.float32)),
        tab,
    )
    cosine, sine = cosine[0:1], sine[0:1]
    q_rot = rotate(by_head(q_in, H), cosine, sine).astype(jnp.bfloat16)
    q_own[...] = q_rot.reshape(2, HALF_H, width)
    k_rot = rotate(by_head(sk_in, KVH), cosine, sine)
    v_own = by_head(sv_in, KVH)
    for half in range(2):
        part = slice(half * HALF_KV, (half + 1) * HALF_KV)
        span_own[half] = jnp.concatenate([k_rot[part], v_own[part]], axis=0)
    slot = lax.broadcasted_iota(jnp.int32, (slots, width), 0)
    pages = jnp.zeros((slots, width), jnp.float32)
    for j in range(slots):
        pages = jnp.where(slot == j, (table_ref[j] * PAGE).astype(jnp.float32), pages)
    pages = jnp.where(slot < counts_ref[0], pages, no_page)
    page_own[...] = pages

    pl.semaphore_wait(barrier, n - 1)

    def q_copy(i):
        peer = forward(i)
        return pltpu.make_async_remote_copy(
            src_ref=q_own.at[lax.rem(peer, 2)], dst_ref=q_all.at[i],
            send_sem=q_send.at[0], recv_sem=q_recv.at[0],
            device_id={"seq": peer}, device_id_type=MESH,
        )

    steps(1, n, lambda i: q_copy(i).start())

    def wait_all(ref, send_sem, recv_sem):
        rest = ref.at[pl.ds(1, n - 1)]
        pltpu.make_async_remote_copy(
            src_ref=rest, dst_ref=rest, send_sem=send_sem.at[0], recv_sem=recv_sem.at[0],
            device_id={"seq": partner}, device_id_type=MESH,
        ).wait()

    def to_partner(src, dst, i):
        return pltpu.make_async_remote_copy(
            src_ref=src, dst_ref=dst, send_sem=peer_send.at[i], recv_sem=peer_recv.at[i],
            device_id={"seq": partner}, device_id_type=MESH,
        )

    other = pl.ds(rows, rows)
    exchange = [
        to_partner(page_own, page_peer, 0),
        to_partner(span_own.at[1 - core], span_peer, 1),
        to_partner(keys_hbm.at[:, theirs], keys_raw.at[other, :], 2),
        to_partner(vals_hbm.at[:, theirs], vals.at[other, :], 3),
    ]
    for copy in exchange:
        copy.start()
    q_all[0] = q_own[core]

    def fill_keys(page_values, base):
        in_page = lax.broadcasted_iota(jnp.int32, (PAGE, width), 0).astype(jnp.float32)
        for j in range(slots):
            at = pl.ds(base + j * PAGE, PAGE)
            c, s = cos_sin(
                jnp.broadcast_to(page_values[j : j + 1], (PAGE, width)), in_page, tab
            )
            for k in range(HALF_KV):
                x = keys_raw[at, k * width : (k + 1) * width].astype(jnp.float32)
                keys_rot[k, at, :] = rotate(x, c, s).astype(jnp.bfloat16)

    def live_bias(page_values):
        wide = jnp.concatenate([page_values] * (rows // width), axis=1)
        lane = lax.broadcasted_iota(jnp.int32, (slots, rows), 1)
        row = lax.broadcasted_iota(jnp.int32, (slots, rows), 0)
        picked = jnp.sum(jnp.where(lane // PAGE == row, wide, 0.0), axis=0, keepdims=True)
        position = picked + lax.rem(lane[0:1], PAGE).astype(jnp.float32)
        return jnp.where(position < start.astype(jnp.float32), 0.0, masked_low)

    own_keys.wait()
    fill_keys(pages, 0)
    bias_own = live_bias(pages)
    own_vals.wait()
    exchange[0].wait()
    exchange[1].wait()
    mine_span = span_own[core]
    peer_span = span_peer[...]
    line = lax.broadcasted_iota(jnp.int32, (SPAN_PAD, width), 0)
    for k in range(HALF_KV):
        for buffer, r in ((0, k), (1, HALF_KV + k)):
            block = jnp.where(
                line == 0, mine_span[r : r + 1],
                jnp.where(line == 1, peer_span[r : r + 1], 0.0),
            ).astype(jnp.bfloat16)
            if buffer == 0:
                keys_rot[k, pl.ds(2 * rows, SPAN_PAD), :] = block
            else:
                vals[pl.ds(2 * rows, SPAN_PAD), k * width : (k + 1) * width] = block
    pages_peer = page_peer[...]
    bias_peer = live_bias(pages_peer)
    exchange[2].wait()
    fill_keys(pages_peer, rows)
    exchange[3].wait()

    bias = jnp.concatenate([bias_own, bias_peer], axis=1)
    count = n
    row_count = count * GROUP
    column = lax.broadcasted_iota(jnp.int32, (row_count, SPAN_PAD), 1)
    lane = lax.broadcasted_iota(jnp.int32, (row_count, width), 1)
    member = lax.rem(lax.broadcasted_iota(jnp.int32, (row_count, width), 0), GROUP)
    own_lane = lax.rem(lane, GROUP) == member
    lane_head = lane // GROUP

    def place(i):
        return lax.rem(i, 2) * chips + i // 2

    def num_copy(i):
        return pltpu.make_async_remote_copy(
            src_ref=num_send.at[i], dst_ref=num_recv.at[place(i)],
            send_sem=num_ss.at[0], recv_sem=num_rs.at[0],
            device_id={"seq": backward(i)}, device_id_type=MESH,
        )

    def stat_copy(i):
        return pltpu.make_async_remote_copy(
            src_ref=stat_send.at[i], dst_ref=stat_recv.at[place(i)],
            send_sem=stat_ss.at[0], recv_sem=stat_rs.at[0],
            device_id={"seq": backward(i)}, device_id_type=MESH,
        )

    def serve(first):
        these = pl.ds(first, count)
        wait_all(q_all, q_send, q_recv)
        token = jnp.concatenate(
            [jnp.full((GROUP, SPAN_PAD), backward(first + i), jnp.int32) for i in range(count)],
            axis=0,
        )
        seen = ((column == 0) & (token >= me)) | ((column == 1) & (token >= partner))
        span_bias = jnp.where(seen, 0.0, masked_low)
        stats = jnp.zeros((row_count, width), jnp.float32)
        for pair in range(HALF_KV // 2):
            both = pl.ds(pair * 2 * GROUP, 2 * GROUP)
            q_pair = q_all[these, both, :].astype(jnp.float32)
            numer = []
            for side in range(2):
                k = pair * 2 + side
                q_one = q_pair[:, side * GROUP : (side + 1) * GROUP, :]
                q_one = q_one.reshape(row_count, width).astype(jnp.bfloat16)
                scores = lax.dot_general(
                    q_one, keys_rot[k, pl.ds(0, 2 * rows), :], (((1,), (1,)), ((), ())),
                    preferred_element_type=jnp.float32,
                ) + bias
                near = lax.dot_general(
                    q_one, keys_rot[k, pl.ds(2 * rows, SPAN_PAD), :], (((1,), (1,)), ((), ())),
                    preferred_element_type=jnp.float32,
                ) + span_bias
                best = jnp.maximum(
                    jnp.max(scores, axis=1, keepdims=True), jnp.max(near, axis=1, keepdims=True)
                )
                w = jnp.exp((scores - best) * factor)
                w_near = jnp.exp((near - best) * factor)
                den = jnp.sum(w, axis=1, keepdims=True) + jnp.sum(w_near, axis=1, keepdims=True)
                at = slice(k * width, (k + 1) * width)
                num = jnp.dot(
                    w.astype(jnp.bfloat16), vals[pl.ds(0, 2 * rows), at],
                    preferred_element_type=jnp.float32,
                ) + jnp.dot(
                    w_near.astype(jnp.bfloat16), vals[pl.ds(2 * rows, SPAN_PAD), at],
                    preferred_element_type=jnp.float32,
                )
                numer.append(num.reshape(count, GROUP, width))
                stats = jnp.where(lane_head == k, best, stats)
                stats = jnp.where(lane_head == HALF_KV + k, den, stats)
            num_send[these, both, :] = jnp.concatenate(numer, axis=1).astype(jnp.bfloat16)
            if pair == HALF_KV // 2 - 1:
                kept = jnp.where(own_lane, stats, 0.0).reshape(count, GROUP, width)
                stat_send[these] = jnp.sum(kept, axis=1, keepdims=True)

    serve(0)

    def answer(i):
        stat_copy(i).start()
        num_copy(i).start()

    steps(1, n, answer)
    num_recv[0] = num_send[0]
    stat_recv[0] = stat_send[0]

    wait_all(stat_recv, stat_ss, stat_rs)
    got = stat_recv[...].reshape(n, width)
    parts = []
    for half in range(2):
        r = got[half * chips : (half + 1) * chips]
        e = jnp.exp((r - jnp.max(r, axis=0, keepdims=True)) * factor)
        d = pltpu.roll(r, width - HALF_H, 1)
        total = jnp.sum(e * d, axis=0, keepdims=True)
        valid = lax.broadcasted_iota(jnp.int32, total.shape, 1) < HALF_H
        parts.append(e / jnp.where(valid, total, 1.0))
    weights = jnp.concatenate(parts, axis=0).T
    pieces = [[], []]
    wait_all(num_recv, num_ss, num_rs)
    for pair in range(HALF_KV // 2):
        both = slice(pair * 2 * GROUP, (pair + 1) * 2 * GROUP)
        acc = [jnp.zeros((2 * GROUP, width), jnp.float32)] * 2
        for i in range(n):
            half = i % 2
            s = half * chips + i // 2
            acc[half] = acc[half] + weights[both, s : s + 1] * num_recv[s, both, :].astype(
                jnp.float32
            )
        for half in range(2):
            pieces[half].append(acc[half])
    same, swapped = (jnp.concatenate(p, axis=0) for p in pieces)
    for half in range(2):
        block = jnp.where(core == half, same, swapped).astype(jnp.bfloat16)
        for h in range(HALF_H):
            at = (half * HALF_H + h) * width
            out_ref[:, at : at + width] = block[h : h + 1]


def body(
    n, queries, span_keys, span_values, cache_keys, cache_values, page_table, page_counts, span_start
):
    assert queries.shape[0] == 1 and n % 2 == 0
    width = queries.shape[1] // H
    rows = cache_keys.shape[0]
    cols = HALF_KV * width
    bf16, f32, i32 = jnp.bfloat16, jnp.float32, jnp.int32
    dma = pltpu.SemaphoreType.DMA
    total = 2 * rows + SPAN_PAD
    return pl.pallas_call(
        functools.partial(kernel, n, width ** (-0.5)),
        out_shape=pltpu.VMEM((1, H * width), bf16),
        in_specs=[pl.BlockSpec(memory_space=pltpu.HBM)] * 9,
        out_specs=pl.BlockSpec(memory_space=pltpu.VMEM),
        scratch_shapes=[
            pltpu.SMEM(page_table.shape, i32),
            pltpu.SMEM((1,), i32),
            pltpu.SMEM((1,), i32),
            pltpu.VMEM((1, H * width), bf16),
            pltpu.VMEM((1, KVH * width), bf16),
            pltpu.VMEM((1, KVH * width), bf16),
            pltpu.VMEM((8, width), f32),
            pltpu.VMEM((2 * rows, cols), bf16),
            pltpu.VMEM((total, cols), bf16),
            pltpu.VMEM((HALF_KV, total, width), bf16),
            pltpu.VMEM((2, HALF_H, width), bf16),
            pltpu.VMEM((n, HALF_H, width), bf16),
            pltpu.VMEM((rows // PAGE, width), f32),
            pltpu.VMEM((rows // PAGE, width), f32),
            pltpu.VMEM((2, 2 * HALF_KV, width), f32),
            pltpu.VMEM((2 * HALF_KV, width), f32),
            pltpu.VMEM((n, HALF_H, width), bf16),
            pltpu.VMEM((n, 1, width), f32),
            pltpu.VMEM((n, HALF_H, width), bf16),
            pltpu.VMEM((n, 1, width), f32),
            dma((9,)), dma((4,)), dma((4,)),
            dma((1,)), dma((1,)), dma((1,)), dma((1,)), dma((1,)), dma((1,)),
        ],
        compiler_params=pltpu.CompilerParams(collective_id=0, has_side_effects=True),
    )(
        page_table, page_counts, span_start, queries, span_keys, span_values,
        jnp.asarray(angle_table(width)), cache_keys, cache_values,
    )


def solution(mesh):
    in_specs = (
        P(("groups", "seq"), None),
        P(("groups", "seq"), None),
        P(("groups", "seq"), None),
        P(("groups", "seq"), None),
        P(("groups", "seq"), None),
        P(("groups", "seq")),
        P(("groups", "seq")),
        P("groups"),
    )
    out_specs = P(("groups", "seq"), None)
    return jax.shard_map(
        functools.partial(body, mesh.shape["seq"]), mesh=mesh, in_specs=in_specs,
        out_specs=out_specs, check_vma=False,
    )
```
